32 devices in a mesh: vocab: 4 (over z), dp: 8 (over y, x, core).
Axes of the slice: x: 2, y: 2, z: 4, core: 2. Of those that a mesh axis runs over, the one named last changes fastest.
Arguments:
- hidden: bfloat16 [2816, 4096], P('dp'), may hold values from -240 to 240
- output_projection_weight: bfloat16 [4096, 16384], P('dp', 'vocab'), may hold values from -0.25 to 0.25
- adapter_down_weight: bfloat16 [4096, 128], replicated, may hold values from -0.09375 to 0.09375
- adapter_up_weight: bfloat16 [128, 16384], P(None, 'vocab'), may hold values from -0.75 to 0.75
- labels: int32 [2816], P('dp'), may hold values from 0 to 16383
- token_job_index: int32 [2816], P('dp'), may hold values from 0 to 7, as said below
Outputs:
- logits: bfloat16 [2816, 16384], P('dp', 'vocab')
- logit_gradient_rows: bfloat16 [2816, 16384], P('dp', 'vocab')
- hidden_state_gradient: bfloat16 [2816, 4096], P('dp')
- token_loss: float32 [2816], P('dp')
- job_loss: float32 [8], replicated
The draws below stay inside these ranges and needn't reach their ends.
Inputs may be any that keep to these rules, and one draw needn't show every extreme that they name: `token_job_index`: a job may have no tokens at all, and the jobs' token counts differ widely.
All inputs are finite; a program needn't handle non-finite values.
Results may differ from the reference program's by a relative error of at most 0.014.
Values may be sent and summed in bfloat16 or wider, within the bound.
No kernel may reach another device: no remote copies, remote signals or barrier semaphores. Data moves between devices by JAX's collectives and lax.ppermute only.
A program may use at most 256 MiB of HBM per device.

```python
import math
import jax
import jax.numpy as jnp
from jax import lax

MODEL_WIDTH = 4096
ADAPTER_JOBS = 8
ADAPTER_RANK = 16
TOKENS = 2816
VOCAB_ENTRIES = 16384


def draw_hidden(key, part):
    values = jnp.clip(jax.random.normal(key, (TOKENS, MODEL_WIDTH), jnp.float32), -6.0, 6.0)
    return values.astype(jnp.bfloat16)


def draw_token_job_index(key, part):
    order_key = jax.random.fold_in(key, 11)
    ticket_key = jax.random.fold_in(key, 12)
    order = jax.random.permutation(order_key, ADAPTER_JOBS).astype(jnp.int32)
    shares = [840 // (place + 1) for place in range(ADAPTER_JOBS - 1)] + [0]
    bounds_list = []
    running = 0
    for share in shares:
        running = running + share
        bounds_list.append(running)
    total_tickets = running
    bounds = jnp.array(bounds_list, dtype=jnp.int32)
    tickets = jax.random.randint(ticket_key, (TOKENS,), 0, total_tickets, dtype=jnp.int32)
    places = jnp.sum((tickets[:, None] >= bounds[None, :]).astype(jnp.int32), axis=1)
    return jnp.take(order, places).astype(jnp.int32)


def touch_ends(values, own_key, smallest, high):
    spot = [jax.random.randint(jax.random.fold_in(own_key, axis), (), 0, length) for axis, length in enumerate(values.shape)]
    main_axis = values.shape.index(max(values.shape))
    next_to = spot[:main_axis] + [(spot[main_axis] + 1) % values.shape[main_axis]] + spot[main_axis + 1:]
    return values.at[tuple(spot)].set(smallest).at[tuple(next_to)].set(high)


def shard_levels(own_key, extent, shards, smallest, high):
    gain, own = 1.0, jax.random.fold_in(own_key, 6)
    for dim, blocks in shards:
        draws = jnp.exp(jax.random.uniform(jax.random.fold_in(own, dim), (blocks,), jnp.float32, smallest / len(shards), high / len(shards)))
        gain = gain * jnp.repeat(draws, extent[dim] // blocks).reshape([-1 if axis == dim else 1 for axis in range(len(extent))])
    return gain


def bell_draw(rng, dims, width, bound, split=(), kind=jnp.bfloat16):
    level = shard_levels(rng, dims, split, -0.22, 0.18) if split else 1.0
    entries = jax.random.normal(rng, dims, jnp.float32) * width * level
    return jnp.minimum(jnp.maximum(entries, -bound), bound).astype(kind)


def setup_inputs(seed: int = 0) -> dict:
    key_list = jax.random.split(jax.random.key(seed), 7)
    return {
        "hidden": draw_hidden(jax.random.fold_in(key_list[6], 71), 0),
        "output_projection_weight": bell_draw(key_list[1], (MODEL_WIDTH, VOCAB_ENTRIES), (MODEL_WIDTH // 9) ** -0.5, 0.25, ((0, 8), (1, 4))),
        "adapter_down_weight": bell_draw(key_list[2], (MODEL_WIDTH, ADAPTER_JOBS * ADAPTER_RANK), MODEL_WIDTH ** -0.5, 0.09375),
        "adapter_up_weight": bell_draw(key_list[3], (ADAPTER_JOBS * ADAPTER_RANK, VOCAB_ENTRIES), (4 * ADAPTER_RANK) ** -0.5, 0.75, ((1, 4),)),
        "labels": touch_ends(jax.random.randint(key_list[4], (TOKENS,), 0, VOCAB_ENTRIES), jax.random.fold_in(key_list[4], 1), 0, VOCAB_ENTRIES - 1).astype(jnp.int32),
        "token_job_index": draw_token_job_index(jax.random.fold_in(key_list[6], 71), 0),
    }


def reference(hidden, output_projection_weight, adapter_down_weight, adapter_up_weight, labels, token_job_index):
    adapter_job_columns = ADAPTER_JOBS * ADAPTER_RANK
    col_job = lax.iota(jnp.int32, adapter_job_columns) // ADAPTER_RANK
    onehot = (token_job_index[:, None] == lax.iota(jnp.int32, ADAPTER_JOBS)[None, :]).astype(jnp.float32)
    counts = jnp.sum(onehot, axis=0)
    per_job = TOKENS / (ADAPTER_JOBS * jnp.maximum(counts, 1.0))
    block = math.gcd(TOKENS, 512)
    steps_count = TOKENS // block

    def one_block(index):
        start = (index * block).astype(jnp.int32)
        hidden_input = lax.dynamic_slice_in_dim(hidden, start, block, 0)
        lab = lax.dynamic_slice_in_dim(labels, start, block, 0)
        jid = lax.dynamic_slice_in_dim(token_job_index, start, block, 0)
        adapter_job_mask = (jid[:, None] == col_job[None, :]).astype(jnp.float32)
        adapter_input = (jnp.dot(hidden_input, adapter_down_weight, preferred_element_type=jnp.float32) * adapter_job_mask).astype(jnp.bfloat16)
        complete_logit_rows = jnp.dot(hidden_input, output_projection_weight, preferred_element_type=jnp.float32) + jnp.dot(adapter_input, adapter_up_weight, preferred_element_type=jnp.float32)
        row_max = jnp.max(complete_logit_rows, axis=1)
        shifted = jnp.exp(complete_logit_rows - row_max[:, None])
        exp_total = jnp.sum(shifted, axis=1)
        target_hit = lax.iota(jnp.int32, VOCAB_ENTRIES)[None, :] == lab[:, None]
        target = jnp.sum(jnp.where(target_hit, complete_logit_rows, 0.0), axis=1)
        token_loss = row_max + jnp.log(exp_total) - target
        token_weight = jnp.sum((jid[:, None] == lax.iota(jnp.int32, ADAPTER_JOBS)[None, :]).astype(jnp.float32) * per_job[None, :], axis=1)
        logit_gradient_rows = (token_weight[:, None] * (shifted / exp_total[:, None] - target_hit.astype(jnp.float32))).astype(jnp.bfloat16)
        adapter_gradient = jnp.dot(logit_gradient_rows, adapter_up_weight.T, preferred_element_type=jnp.float32)
        hidden_state_gradient = jnp.dot(logit_gradient_rows, output_projection_weight.T, preferred_element_type=jnp.float32) + jnp.dot(adapter_gradient * adapter_job_mask, adapter_down_weight.astype(jnp.float32).T, precision=lax.Precision.HIGHEST)
        return complete_logit_rows.astype(jnp.bfloat16), logit_gradient_rows, hidden_state_gradient.astype(jnp.bfloat16), token_loss

    logits, logit_gradient_rows, hidden_state_gradient, token_loss = lax.map(one_block, jnp.arange(steps_count, dtype=jnp.int32))
    logits = logits.reshape(TOKENS, VOCAB_ENTRIES)
    logit_gradient_rows = logit_gradient_rows.reshape(TOKENS, VOCAB_ENTRIES)
    hidden_state_gradient = hidden_state_gradient.reshape(TOKENS, MODEL_WIDTH)
    token_loss = token_loss.reshape(TOKENS)
    job_loss = jnp.sum(onehot * token_loss[:, None], axis=0) / jnp.maximum(counts, 1.0)
    return logits, logit_gradient_rows, hidden_state_gradient, token_loss, job_loss
```

```python
import jax
import jax.numpy as jnp
from jax import lax
from jax.experimental import pallas as pl
from jax.experimental.pallas import tpu as pltpu
from jax.sharding import PartitionSpec as P


ADAPTER_JOBS = 8
ADAPTER_RANK = 16
BF = jnp.bfloat16
F32 = jnp.float32
NT = (((1,), (1,)), ((), ()))


def dot_nt(a, b):
    return lax.dot_general(a, b, NT, preferred_element_type=F32)


def swap(x, axis, n, bit):
    return lax.ppermute(x, axis, [(i, i ^ bit) for i in range(n)])


def params(mib=40):
    return pltpu.CompilerParams(vmem_limit_bytes=mib * 1024 * 1024)


def whole(shape):
    return pl.BlockSpec(shape, lambda *_: (0,) * len(shape))


def stacked(refs):
    parts = [r[...] for r in refs]
    return parts[0] if len(parts) == 1 else jnp.concatenate(parts, axis=0)


def wide_runs(refs):
    runs, run, at = [], [], 0
    for ref in refs:
        run.append(ref)
        size = sum(r.shape[0] for r in run)
        if size >= 256 or ref is refs[-1]:
            runs.append((at, size, run))
            at += size
            run = []
    return runs


def one_hot(label, j, t, bv):
    return lax.broadcasted_iota(jnp.int32, (t, bv), 1) + j * bv == label


def halves(w):
    rows, v = w.shape
    bv = min(1024, v)

    def body(w_ref, low_ref, high_ref):
        low_ref[...] = w_ref[:rows // 2]
        high_ref[...] = w_ref[rows // 2:]

    return pl.pallas_call(
        body,
        grid=(v // bv,),
        in_specs=[pl.BlockSpec((rows, bv), lambda j: (0, j))],
        out_specs=[pl.BlockSpec((rows // 2, bv), lambda j: (0, j))] * 2,
        out_shape=[jax.ShapeDtypeStruct((rows // 2, v), w.dtype)] * 2,
        compiler_params=params(),
        name="halves",
        cost_estimate=pl.CostEstimate(flops=rows * v, bytes_accessed=4 * rows * v, transcendentals=0),
    )(w)


def forward_group(acc, h, pieces, extra):
    t, v = h.shape[0], pieces[0].shape[1]
    bv = min(512, v)
    total = sum(p.shape[0] for p in pieces)
    first = acc is None

    def body(*refs):
        refs = list(refs)
        acc_ref = None if first else refs.pop(0)
        h_ref = refs.pop(0)
        ex = (refs.pop(0), refs.pop(0)) if extra is not None else None
        piece_refs, o_ref = refs[: len(pieces)], refs[-1]
        out = jnp.dot(h_ref[...], stacked(piece_refs), preferred_element_type=F32)
        if not first:
            out = out + acc_ref[...]
        if ex is not None:
            out = out + jnp.dot(ex[0][...], ex[1][...], preferred_element_type=F32)
        o_ref[...] = out

    col = pl.BlockSpec((t, bv), lambda j: (0, j))
    in_specs = [] if first else [col]
    args = [] if first else [acc]
    in_specs.append(whole((t, total)))
    args.append(h)
    if extra is not None:
        rank = extra[1].shape[0]
        in_specs += [whole((t, rank)), pl.BlockSpec((rank, bv), lambda j: (0, j))]
        args += list(extra)
    for p in pieces:
        in_specs.append(pl.BlockSpec((p.shape[0], bv), lambda j: (0, j)))
    return pl.pallas_call(
        body,
        grid=(v // bv,),
        in_specs=in_specs,
        out_specs=col,
        out_shape=jax.ShapeDtypeStruct((t, v), F32),
        compiler_params=params(),
        cost_estimate=pl.CostEstimate(
            flops=2 * t * v * total, bytes_accessed=2 * total * v + 8 * t * v, transcendentals=0
        ),
    )(*args, *pieces)


def finish_forward(acc, h, pieces, label, wide):
    t, v = acc.shape
    bv = min(2048, v)
    nb = v // bv
    total = sum(p.shape[0] for p in pieces)

    def body(acc_ref, h_ref, lab_ref, *refs):
        piece_refs = refs[: len(pieces)]
        logit_ref, e_ref, stat_ref, full, top, sums, hit = refs[len(pieces):]
        phase, j = pl.program_id(0), pl.program_id(1)
        here = pl.ds(pl.multiple_of(j * bv, bv), bv)
        is_label = one_hot(lab_ref[...], j, t, bv)

        @pl.when(phase == 0)
        def _():
            @pl.when(j == 0)
            def _():
                top[...] = jnp.full_like(top, -jnp.inf)
                hit[...] = jnp.zeros_like(hit)
                sums[...] = jnp.zeros_like(sums)

            out = acc_ref[...] + jnp.dot(
                h_ref[...], stacked(piece_refs), preferred_element_type=F32
            )
            full[:, here] = out
            logit_ref[...] = out.astype(BF)
            best, got = top[...], hit[...]
            kept = jnp.where(is_label, out, 0.0)
            for k in range(0, bv, 128):
                best = jnp.maximum(best, out[:, k:k + 128])
                got = got + kept[:, k:k + 128]
            top[...] = best
            hit[...] = got

        @pl.when(phase == 1)
        def _():
            @pl.when(j == 0)
            def _():
                top[...] = jnp.broadcast_to(jnp.max(top[...], axis=1, keepdims=True), top.shape)

            e = jnp.exp(full[:, here] - top[:, :1])
            acc_sum = sums[...]
            for k in range(0, bv, 128):
                acc_sum = acc_sum + e[:, k:k + 128]
            sums[...] = acc_sum
            e_ref[...] = jnp.where(is_label, 0.0, e).astype(BF)

            @pl.when(j == nb - 1)
            def _():
                lane = lax.broadcasted_iota(jnp.int32, (t, 128), 1)
                s = jnp.sum(acc_sum, axis=1, keepdims=True)
                g = jnp.sum(hit[...], axis=1, keepdims=True)
                terms = jnp.where(lane == 0, top[...], jnp.where(lane == 1, s, g))
                if wide > t:
                    terms = jnp.concatenate([terms, jnp.zeros((wide - t, 128), F32)], axis=0)
                stat_ref[...] = terms.T[:8, :]

    def walk(p, j):
        return (0, jnp.where(p == 0, j, nb - 1))

    def walk2(p, j):
        return (0, jnp.where(p == 0, 0, j))

    return pl.pallas_call(
        body,
        grid=(2, nb),
        in_specs=[
            pl.BlockSpec((t, bv), walk),
            whole((t, total)),
            whole((t, 1)),
        ] + [pl.BlockSpec((p.shape[0], bv), walk) for p in pieces],
        out_specs=[
            pl.BlockSpec((t, bv), walk),
            pl.BlockSpec((t, bv), walk2),
            whole((8, wide)),
        ],
        out_shape=[
            jax.ShapeDtypeStruct((t, v), BF),
            jax.ShapeDtypeStruct((t, v), BF),
            jax.ShapeDtypeStruct((8, wide), F32),
        ],
        scratch_shapes=[pltpu.VMEM((t, v), F32)] + [pltpu.VMEM((t, 128), F32)] * 3,
        compiler_params=params(48),
        name="finish_forward",
        cost_estimate=pl.CostEstimate(
            flops=2 * t * v * total + 40 * t * v, bytes_accessed=2 * total * v + 8 * t * v,
            transcendentals=t * v,
        ),
    )(acc, h, label, *pieces)


def gradient_and_chunks(e, label, own, joint, weight, up, mask, pieces, down, sizes):
    t, v = e.shape
    bv = min(2048, v)
    nb = v // bv
    rank = up.shape[0]
    wide = own.shape[1]
    total = sum(p.shape[0] for p in pieces)

    def body(own_ref, all_ref, weight_ref, mask_ref, down_ref, e_ref, lab_ref, up_ref, *refs):
        piece_refs = refs[: len(pieces)]
        grad_ref, lg_ref, *outs, cols, g, sums = refs[len(pieces):]
        j = pl.program_id(0)

        @pl.when(j == 0)
        def _():
            row = lax.broadcasted_iota(jnp.int32, (128, wide), 0)
            total_exp = all_ref[1:2, :]
            w = weight_ref[0:1, :]
            scale = w * (jnp.exp(own_ref[0:1, :] - all_ref[0:1, :]) / total_exp)
            at_label = w * (jnp.exp(all_ref[2:3, :] - all_ref[0:1, :]) / total_exp - 1.0)
            cols[...] = jnp.where(row == 0, scale, at_label).T[:t, :]
            g[...] = jnp.zeros_like(g)
            sums[...] = jnp.zeros_like(sums)

        scaled = cols[:, 0:1] * e_ref[...].astype(F32)
        rows = jnp.where(one_hot(lab_ref[...], j, t, bv), cols[:, 1:2], scaled).astype(BF)
        grad_ref[...] = rows
        g[...] += dot_nt(rows, up_ref[...])
        for at, size, run in wide_runs(piece_refs):
            sums[:, at:at + size] += dot_nt(rows, stacked(run))

        @pl.when(j == nb - 1)
        def _():
            lg = g[...] * mask_ref[...]
            for k in range(3):
                part = lg.astype(BF)
                lg_ref[:, k * rank:(k + 1) * rank] = part
                lg = lg - part.astype(F32)
            lo = 0
            for size, o in zip(sizes, outs):
                out = sums[:, lo:lo + size] + dot_nt(lg_ref[...], down_ref[lo:lo + size, :])
                o[...] = out.astype(BF)
                lo += size

    col = pl.BlockSpec((t, bv), lambda j: (0, j))
    small = [own, joint, weight, mask, down]
    return pl.pallas_call(
        body,
        grid=(nb,),
        in_specs=[whole(a.shape) for a in small]
        + [col, whole((t, 1)), pl.BlockSpec((rank, bv), lambda j: (0, j))]
        + [pl.BlockSpec((p.shape[0], bv), lambda j: (0, j)) for p in pieces],
        out_specs=[col, whole((t, 3 * rank))] + [whole((t, size)) for size in sizes],
        out_shape=[
            jax.ShapeDtypeStruct((t, v), BF),
            jax.ShapeDtypeStruct((t, 3 * rank), BF),
        ] + [jax.ShapeDtypeStruct((t, size), BF) for size in sizes],
        scratch_shapes=[
            pltpu.VMEM((t, 128), F32), pltpu.VMEM((t, rank), F32), pltpu.VMEM((t, total), F32),
        ],
        compiler_params=params(),
        name="gradient_first",
        cost_estimate=pl.CostEstimate(
            flops=2 * t * v * (total + rank), bytes_accessed=2 * (total + 2 * t) * v,
            transcendentals=0,
        ),
    )(*small, e, label, up, *pieces)


def column_chunks(grad, lg, pieces, down, sizes):
    t, v = grad.shape
    bv = min(2048, v)
    nb = v // bv
    total = down.shape[0]

    def body(grad_ref, lg_ref, down_ref, *refs):
        piece_refs = refs[: len(pieces)]
        outs, sums = refs[len(pieces):-1], refs[-1]
        j = pl.program_id(0)

        @pl.when(j == 0)
        def _():
            sums[...] = jnp.zeros_like(sums)

        for at, size, run in wide_runs(piece_refs):
            sums[:, at:at + size] += dot_nt(grad_ref[...], stacked(run))

        @pl.when(j == nb - 1)
        def _():
            lo = 0
            for size, o in zip(sizes, outs):
                out = sums[:, lo:lo + size] + dot_nt(lg_ref[...], down_ref[lo:lo + size, :])
                o[...] = out.astype(BF)
                lo += size

    return pl.pallas_call(
        body,
        grid=(nb,),
        in_specs=[
            pl.BlockSpec((t, bv), lambda j: (0, j)), whole(lg.shape), whole(down.shape),
        ] + [pl.BlockSpec((p.shape[0], bv), lambda j: (0, j)) for p in pieces],
        out_specs=[whole((t, size)) for size in sizes],
        out_shape=[jax.ShapeDtypeStruct((t, size), BF) for size in sizes],
        scratch_shapes=[pltpu.VMEM((t, total), F32)],
        compiler_params=params(),
        cost_estimate=pl.CostEstimate(
            flops=2 * t * v * total, bytes_accessed=2 * (total + t) * v, transcendentals=0
        ),
    )(grad, lg, down, *pieces)


def gather_plan(n, rows):
    half, q = rows // 2, rows // 4
    evens = sorted(range(2, n, 2), key=lambda r: (bin(r).count("1"), r))
    singles = [r for r in evens if bin(r).count("1") == 1]
    multi = [r for r in evens if bin(r).count("1") > 1]
    lists = [[(0, 0, rows)]]
    for turn in range(2):
        lists.append([(r, half * ((i + turn + 1) % 2), half) for i, r in enumerate(singles)])
    for r in multi[:-1]:
        lists.append([(r, 0, half), (r, half, half)])
    for r in multi[-1:]:
        for s in (0, q):
            lists.append([(r, s, q), (r, half + s, q)])
    return [some + [(r + 1, s, l) for r, s, l in some if n > 1] for some in lists if some]


def chunk_plan(groups, rows):
    flat = [p for group in groups for p in group]
    runs, run = [], []
    for p in flat:
        run.append(p)
        if sum(q[2] for q in run) >= (rows if len(runs) < 2 else 3 * rows // 2):
            runs.append(run)
            run = []
    if run:
        runs.append(run)
    shares = [[0]] + [list(range(k, min(k + 2, len(runs)))) for k in range(1, len(runs), 2)]
    return runs, shares


def program(hidden, w_own, down, up, labels, token_job_index):
    n, m = lax.axis_size("dp"), lax.axis_size("vocab")
    me, z = lax.axis_index("dp"), lax.axis_index("vocab")
    t, width = hidden.shape
    rows, v = w_own.shape
    rank = down.shape[1]
    half = rows // 2
    wide = -(-t // 128) * 128

    groups = gather_plan(n, rows)
    have = {(0, 0, rows): w_own}
    low, high = halves(w_own)
    own_halves = {half: high, 0: low}

    def part_of(r, s, length):
        if r == 0 and length == half:
            return own_halves[s]
        if (r, s, length) in have:
            return have[(r, s, length)]
        for (r2, s2, l2), arr in have.items():
            if r2 == r and s2 <= s and s + length <= s2 + l2:
                return lax.slice_in_dim(arr, s - s2, s - s2 + length, axis=0)

    for group in groups:
        for r, s, length in group:
            if r % 2 == 0 and r:
                bit = r & -r if s < half else 1 << (r.bit_length() - 1)
                src = part_of(r ^ bit, s, length)
                have[(r, s, length)] = swap(src, "dp", n, bit)
        for r, s, length in group:
            if r % 2:
                src = part_of(r ^ 1, s, length)
                have[(r, s, length)] = swap(src, "dp", n, 1)

    onehot = (token_job_index[:, None] == lax.iota(jnp.int32, ADAPTER_JOBS)[None, :]).astype(F32)
    counts = jnp.sum(onehot, axis=0)
    bits = [1 << b for b in range(n.bit_length() - 1)]
    for bit in bits[:1] + bits[:0:-1]:
        other = swap(counts, "dp", n, bit)
        counts = counts + other
    per_job = t * n / (ADAPTER_JOBS * jnp.maximum(counts, 1.0))
    token_weight = jnp.sum(onehot * per_job[None, :], axis=1)
    weight = jnp.broadcast_to(jnp.pad(token_weight, (0, wide - t))[None, :], (8, wide))

    def columns(x, group, axis):
        return jnp.concatenate(
            [lax.dynamic_slice_in_dim(x, (me ^ r) * rows + s, length, axis) for r, s, length in group],
            axis=axis,
        )

    runs, shares = chunk_plan(groups, rows)
    local_label = (labels - z * v)[:, None]
    mask = (token_job_index[:, None] == lax.iota(jnp.int32, rank)[None, :] // ADAPTER_RANK).astype(F32)
    hs = [columns(hidden, group, 1) for group in groups]
    downs = [columns(down, [p for c in share for p in runs[c]], 0) for share in shares]
    downs = [jnp.concatenate([d] * 3, axis=1) for d in downs]
    lora_in = (jnp.dot(hidden, down, preferred_element_type=F32) * mask).astype(BF)
    hs, downs, mask, onehot, lora_in, local_label = lax.optimization_barrier(
        (hs, downs, mask, onehot, lora_in, local_label)
    )

    acc = None
    for k, group in enumerate(groups[:-1]):
        acc = forward_group(acc, hs[k], [have[p] for p in group], (lora_in, up) if k == 0 else None)
    acc, weight = lax.optimization_barrier((acc, weight))
    logits, e, own = finish_forward(acc, hs[-1], [have[p] for p in groups[-1]], local_label, wide)

    def join(a, b):
        top = jnp.maximum(a[0:1], b[0:1])
        s = a[1:2] * jnp.exp(a[0:1] - top) + b[1:2] * jnp.exp(b[0:1] - top)
        return jnp.concatenate([top, s, a[2:3] + b[2:3], jnp.zeros((5, wide), F32)], axis=0)

    joint, bit = own, 1
    while bit < m:
        other = swap(joint, "vocab", m, bit)
        joint = join(joint, other)
        bit *= 2
    row_max, exp_total, target = joint[0, :t], joint[1, :t], joint[2, :t]
    token_loss = row_max + jnp.log(exp_total) - target

    terms = []
    for k, share in enumerate(shares):
        pieces = [have[p] for c in share for p in runs[c]]
        sizes = [sum(p[2] for p in runs[c]) for c in share]
        if k == 0:
            grad, lg, *terms = gradient_and_chunks(
                e, local_label, own, joint, weight, up, mask, pieces, downs[0], sizes
            )
        else:
            terms += column_chunks(grad, lg, pieces, downs[k], sizes)

    inward = m // 2 - 1
    out = jnp.zeros((t, width), BF)
    for part, run in zip(terms, runs):
        for s in range(inward):
            got = lax.ppermute(part, "vocab", [(s, s + 1), (m - 1 - s, m - 2 - s)])
            part = part + got
        got = lax.ppermute(part, "vocab", [(m // 2 - 1, m // 2), (m // 2, m // 2 - 1)])
        part = part + got
        for s in reversed(range(inward)):
            got = lax.ppermute(part, "vocab", [(s + 1, s), (m - 2 - s, m - 1 - s)])
            part = jnp.where((z == s) | (z == m - 1 - s), got, part)
        at = 0
        for r, s, length in run:
            out = lax.dynamic_update_slice_in_dim(
                out, part[:, at:at + length], (me ^ r) * rows + s, axis=1
            )
            at += length

    job_sums = jnp.sum(onehot * token_loss[:, None], axis=0)
    for bit in bits[:1] + bits[:0:-1]:
        other = swap(job_sums, "dp", n, bit)
        job_sums = job_sums + other
    job_sums, counts = lax.optimization_barrier((job_sums, counts))
    job_loss = job_sums / jnp.maximum(counts, 1.0)
    return logits, grad, out, token_loss, job_loss


def solution(mesh):
    in_specs = (P("dp", None), P("dp", "vocab"), P(), P(None, "vocab"), P("dp"), P("dp"))
    out_specs = (P("dp", "vocab"), P("dp", "vocab"), P("dp", None), P("dp"), P())
    return jax.shard_map(program, mesh=mesh, in_specs=in_specs, out_specs=out_specs, check_vma=False)
```

```python
import jax
import jax.numpy as jnp
from jax import lax
from jax.experimental import pallas as pl
from jax.experimental.pallas import tpu as pltpu
from jax.sharding import PartitionSpec as P


ADAPTER_JOBS = 8
ADAPTER_RANK = 16
BF = jnp.bfloat16
F32 = jnp.float32
NT = (((1,), (1,)), ((), ()))


def dot_nt(a, b):
    return lax.dot_general(a, b, NT, preferred_element_type=F32)


def swap(x, axis, n, bit):
    return lax.ppermute(x, axis, [(i, i ^ bit) for i in range(n)])


def params(mib=26):
    return pltpu.CompilerParams(vmem_limit_bytes=mib * 1024 * 1024)


def whole(shape):
    return pl.BlockSpec(shape, lambda *_: (0,) * len(shape))


def stacked(refs):
    parts = [r[...] for r in refs]
    return parts[0] if len(parts) == 1 else jnp.concatenate(parts, axis=0)


def wide_runs(refs):
    runs, run, at = [], [], 0
    for ref in refs:
        run.append(ref)
        size = sum(r.shape[0] for r in run)
        if size >= 256 or ref is refs[-1]:
            runs.append((at, size, run))
            at += size
            run = []
    return runs


def one_hot(label, j, t, bv):
    return lax.broadcasted_iota(jnp.int32, (t, bv), 1) + j * bv == label


def halves(w):
    rows, v = w.shape
    bv = min(2048, v)

    def body(w_ref, low_ref, high_ref):
        low_ref[...] = w_ref[:rows // 2]
        high_ref[...] = w_ref[rows // 2:]

    return pl.pallas_call(
        body,
        grid=(v // bv,),
        in_specs=[pl.BlockSpec((rows, bv), lambda j: (0, j))],
        out_specs=[pl.BlockSpec((rows // 2, bv), lambda j: (0, j))] * 2,
        out_shape=[jax.ShapeDtypeStruct((rows // 2, v), w.dtype)] * 2,
        compiler_params=params(),
        name="halves",
        cost_estimate=pl.CostEstimate(flops=rows * v, bytes_accessed=4 * rows * v, transcendentals=0),
    )(w)


def forward_group(acc, h, pieces, extra):
    t, v = h.shape[0], pieces[0].shape[1]
    bv = min(512, v)
    total = sum(p.shape[0] for p in pieces)
    first = acc is None

    def body(*refs):
        refs = list(refs)
        acc_ref = None if first else refs.pop(0)
        h_ref = refs.pop(0)
        ex = (refs.pop(0), refs.pop(0)) if extra is not None else None
        piece_refs, o_ref = refs[: len(pieces)], refs[-1]
        out = jnp.dot(h_ref[...], stacked(piece_refs), preferred_element_type=F32)
        if not first:
            out = out + acc_ref[...]
        if ex is not None:
            out = out + jnp.dot(ex[0][...], ex[1][...], preferred_element_type=F32)
        o_ref[...] = out

    col = pl.BlockSpec((t, bv), lambda j: (0, j))
    in_specs = [] if first else [col]
    args = [] if first else [acc]
    in_specs.append(whole((t, total)))
    args.append(h)
    if extra is not None:
        rank = extra[1].shape[0]
        in_specs += [whole((t, rank)), pl.BlockSpec((rank, bv), lambda j: (0, j))]
        args += list(extra)
    for p in pieces:
        in_specs.append(pl.BlockSpec((p.shape[0], bv), lambda j: (0, j)))
    return pl.pallas_call(
        body,
        grid=(v // bv,),
        in_specs=in_specs,
        out_specs=col,
        out_shape=jax.ShapeDtypeStruct((t, v), F32),
        compiler_params=params(),
        cost_estimate=pl.CostEstimate(
            flops=2 * t * v * total, bytes_accessed=2 * total * v + 8 * t * v, transcendentals=0
        ),
    )(*args, *pieces)


def finish_forward(acc, h, pieces, label, weight):
    t, v = acc.shape
    wide = weight.shape[1]
    bv = min(2048, v)
    nb = v // bv
    total = sum(p.shape[0] for p in pieces)

    def body(acc_ref, h_ref, lab_ref, weight_ref, *refs):
        piece_refs = refs[: len(pieces)]
        logit_ref, e_ref, stat_ref, full, top, sums, hit = refs[len(pieces):]
        phase, j = pl.program_id(0), pl.program_id(1)
        here = pl.ds(pl.multiple_of(j * bv, bv), bv)
        is_label = one_hot(lab_ref[...], j, t, bv)

        @pl.when(phase == 0)
        def _():
            @pl.when(j == 0)
            def _():
                top[...] = jnp.full_like(top, -jnp.inf)
                hit[...] = jnp.zeros_like(hit)
                sums[...] = jnp.zeros_like(sums)

            out = acc_ref[...] + jnp.dot(
                h_ref[...], stacked(piece_refs), preferred_element_type=F32
            )
            full[:, here] = out
            logit_ref[...] = out.astype(BF)
            best, got = top[...], hit[...]
            kept = jnp.where(is_label, out, 0.0)
            for k in range(0, bv, 128):
                best = jnp.maximum(best, out[:, k:k + 128])
                got = got + kept[:, k:k + 128]
            top[...] = best
            hit[...] = got

        @pl.when(phase == 1)
        def _():
            @pl.when(j == 0)
            def _():
                top[...] = jnp.broadcast_to(jnp.max(top[...], axis=1, keepdims=True), top.shape)

            e = jnp.exp(full[:, here] - top[:, :1])
            acc_sum = sums[...]
            for k in range(0, bv, 128):
                acc_sum = acc_sum + e[:, k:k + 128]
            sums[...] = acc_sum
            e_ref[...] = jnp.where(is_label, 0.0, e).astype(BF)

            @pl.when(j == nb - 1)
            def _():
                lane = lax.broadcasted_iota(jnp.int32, (t, 128), 1)
                s = jnp.sum(acc_sum, axis=1, keepdims=True)
                g = jnp.sum(hit[...], axis=1, keepdims=True)
                terms = jnp.where(lane == 0, top[...], jnp.where(lane == 1, s, g))
                if wide > t:
                    terms = jnp.concatenate([terms, jnp.zeros((wide - t, 128), F32)], axis=0)
                row = lax.broadcasted_iota(jnp.int32, (8, wide), 0)
                stat_ref[...] = jnp.where(row == 3, weight_ref[...], terms.T[:8, :])

    def walk(p, j):
        return (0, jnp.where(p == 0, j, nb - 1))

    def walk2(p, j):
        return (0, jnp.where(p == 0, 0, j))

    return pl.pallas_call(
        body,
        grid=(2, nb),
        in_specs=[
            pl.BlockSpec((t, bv), walk),
            whole((t, total)),
            whole((t, 1)),
            whole((8, wide)),
        ] + [pl.BlockSpec((p.shape[0], bv), walk) for p in pieces],
        out_specs=[
            pl.BlockSpec((t, bv), walk),
            pl.BlockSpec((t, bv), walk2),
            whole((8, wide)),
        ],
        out_shape=[
            jax.ShapeDtypeStruct((t, v), BF),
            jax.ShapeDtypeStruct((t, v), BF),
            jax.ShapeDtypeStruct((8, wide), F32),
        ],
        scratch_shapes=[pltpu.VMEM((t, v), F32)] + [pltpu.VMEM((t, 128), F32)] * 3,
        compiler_params=params(28),
        name="finish_forward",
        cost_estimate=pl.CostEstimate(
            flops=2 * t * v * total + 40 * t * v, bytes_accessed=2 * total * v + 8 * t * v,
            transcendentals=t * v,
        ),
    )(acc, h, label, weight, *pieces)


def gradient_and_chunks(e, label, own, joint, up, mask, pieces, down, sizes):
    t, v = e.shape
    bv = min(2048, v)
    nb = v // bv
    rank = up.shape[0]
    wide = own.shape[1]
    total = sum(p.shape[0] for p in pieces)

    def body(own_ref, all_ref, mask_ref, down_ref, e_ref, lab_ref, up_ref, *refs):
        piece_refs = refs[: len(pieces)]
        grad_ref, again_ref, lg_ref, *outs, cols, g, sums = refs[len(pieces):]
        j = pl.program_id(0)

        @pl.when(j == 0)
        def _():
            row = lax.broadcasted_iota(jnp.int32, (128, wide), 0)
            total_exp = all_ref[1:2, :]
            w = own_ref[3:4, :]
            scale = w * (jnp.exp(own_ref[0:1, :] - all_ref[0:1, :]) / total_exp)
            at_label = w * (jnp.exp(all_ref[2:3, :] - all_ref[0:1, :]) / total_exp - 1.0)
            cols[...] = jnp.where(row == 0, scale, at_label).T[:t, :]
            g[...] = jnp.zeros_like(g)
            sums[...] = jnp.zeros_like(sums)

        scaled = cols[:, 0:1] * e_ref[...].astype(F32)
        rows = jnp.where(one_hot(lab_ref[...], j, t, bv), cols[:, 1:2], scaled).astype(BF)
        grad_ref[...] = rows
        again_ref[...] = rows
        g[...] += dot_nt(rows, up_ref[...])
        for at, size, run in wide_runs(piece_refs):
            sums[:, at:at + size] += dot_nt(rows, stacked(run))

        @pl.when(j == nb - 1)
        def _():
            lg = g[...] * mask_ref[...]
            for k in range(3):
                part = lg.astype(BF)
                lg_ref[:, k * rank:(k + 1) * rank] = part
                lg = lg - part.astype(F32)
            lo = 0
            for size, o in zip(sizes, outs):
                out = sums[:, lo:lo + size] + dot_nt(lg_ref[...], down_ref[lo:lo + size, :])
                o[...] = out.astype(BF)
                lo += size

    col = pl.BlockSpec((t, bv), lambda j: (0, j))
    small = [own, joint, mask, down]
    return pl.pallas_call(
        body,
        grid=(nb,),
        in_specs=[whole(a.shape) for a in small]
        + [col, whole((t, 1)), pl.BlockSpec((rank, bv), lambda j: (0, j))]
        + [pl.BlockSpec((p.shape[0], bv), lambda j: (0, j)) for p in pieces],
        out_specs=[col, col, whole((t, 3 * rank))] + [whole((t, size)) for size in sizes],
        out_shape=[
            jax.ShapeDtypeStruct((t, v), BF),
            jax.ShapeDtypeStruct((t, v), BF),
            jax.ShapeDtypeStruct((t, 3 * rank), BF),
        ] + [jax.ShapeDtypeStruct((t, size), BF) for size in sizes],
        scratch_shapes=[
            pltpu.VMEM((t, 128), F32), pltpu.VMEM((t, rank), F32), pltpu.VMEM((t, total), F32),
        ],
        compiler_params=params(26),
        name="gradient_first",
        cost_estimate=pl.CostEstimate(
            flops=2 * t * v * (total + rank), bytes_accessed=2 * (total + 2 * t) * v,
            transcendentals=0,
        ),
    )(*small, e, label, up, *pieces)


def column_chunks(grad, lg, pieces, down, sizes):
    t, v = grad.shape
    bv = min(2048, v)
    nb = v // bv
    total = down.shape[0]

    def body(grad_ref, lg_ref, down_ref, *refs):
        piece_refs = refs[: len(pieces)]
        outs, sums = refs[len(pieces):-1], refs[-1]
        j = pl.program_id(0)

        @pl.when(j == 0)
        def _():
            sums[...] = jnp.zeros_like(sums)

        for at, size, run in wide_runs(piece_refs):
            sums[:, at:at + size] += dot_nt(grad_ref[...], stacked(run))

        @pl.when(j == nb - 1)
        def _():
            lo = 0
            for size, o in zip(sizes, outs):
                out = sums[:, lo:lo + size] + dot_nt(lg_ref[...], down_ref[lo:lo + size, :])
                o[...] = out.astype(BF)
                lo += size

    return pl.pallas_call(
        body,
        grid=(nb,),
        in_specs=[
            pl.BlockSpec((t, bv), lambda j: (0, j)), whole(lg.shape), whole(down.shape),
        ] + [pl.BlockSpec((p.shape[0], bv), lambda j: (0, j)) for p in pieces],
        out_specs=[whole((t, size)) for size in sizes],
        out_shape=[jax.ShapeDtypeStruct((t, size), BF) for size in sizes],
        scratch_shapes=[pltpu.VMEM((t, total), F32)],
        compiler_params=params(26),
        cost_estimate=pl.CostEstimate(
            flops=2 * t * v * total, bytes_accessed=2 * (total + t) * v, transcendentals=0
        ),
    )(grad, lg, down, *pieces)


def gather_plan(n, rows):
    half, q = rows // 2, rows // 4
    evens = sorted(range(2, n, 2), key=lambda r: (bin(r).count("1"), r))
    singles = [r for r in evens if bin(r).count("1") == 1]
    multi = [r for r in evens if bin(r).count("1") > 1]
    lists = [[(0, 0, rows)]]
    for turn in range(2):
        lists.append([(r, half * ((i + turn + 1) % 2), half) for i, r in enumerate(singles)])
    for r in multi[:-1]:
        lists.append([(r, 0, half), (r, half, half)])
    for r in multi[-1:]:
        for s in (0, q):
            lists.append([(r, s, q), (r, half + s, q)])
    return [some + [(r + 1, s, l) for r, s, l in some if n > 1] for some in lists if some]


def chunk_plan(groups, rows):
    flat = [p for group in groups for p in group]
    runs, run = [], []
    for p in flat:
        run.append(p)
        if sum(q[2] for q in run) >= rows:
            runs.append(run)
            run = []
    if run:
        runs.append(run)
    shares = [[0]] + [list(range(k, min(k + 2, len(runs)))) for k in range(1, len(runs), 2)]
    return runs, shares


def program(hidden, w_own, down, up, labels, token_job_index):
    n, m = lax.axis_size("dp"), lax.axis_size("vocab")
    me, z = lax.axis_index("dp"), lax.axis_index("vocab")
    t, width = hidden.shape
    rows, v = w_own.shape
    rank = down.shape[1]
    half = rows // 2
    wide = -(-t // 128) * 128

    groups = gather_plan(n, rows)
    have = {(0, 0, rows): w_own}
    low, high = halves(w_own)
    own_halves = {half: high, 0: low}

    def part_of(r, s, length):
        if r == 0 and length == half:
            return own_halves[s]
        if (r, s, length) in have:
            return have[(r, s, length)]
        for (r2, s2, l2), arr in have.items():
            if r2 == r and s2 <= s and s + length <= s2 + l2:
                return lax.slice_in_dim(arr, s - s2, s - s2 + length, axis=0)

    for group in groups:
        for r, s, length in group:
            if r % 2 == 0 and r:
                bit = r & -r if s < half else 1 << (r.bit_length() - 1)
                src = part_of(r ^ bit, s, length)
                have[(r, s, length)] = swap(src, "dp", n, bit)
        for r, s, length in group:
            if r % 2:
                src = part_of(r ^ 1, s, length)
                have[(r, s, length)] = swap(src, "dp", n, 1)

    onehot = (token_job_index[:, None] == lax.iota(jnp.int32, ADAPTER_JOBS)[None, :]).astype(F32)
    counts = jnp.sum(onehot, axis=0)
    bits = [1 << b for b in range(n.bit_length() - 1)]
    for bit in bits[:1] + bits[:0:-1]:
        other = swap(counts, "dp", n, bit)
        counts = counts + other
    per_job = t * n / (ADAPTER_JOBS * jnp.maximum(counts, 1.0))
    token_weight = jnp.sum(onehot * per_job[None, :], axis=1)
    weight = jnp.broadcast_to(jnp.pad(token_weight, (0, wide - t))[None, :], (8, wide))

    def columns(x, group, axis):
        return jnp.concatenate(
            [lax.dynamic_slice_in_dim(x, (me ^ r) * rows + s, length, axis) for r, s, length in group],
            axis=axis,
        )

    runs, shares = chunk_plan(groups, rows)
    local_label = (labels - z * v)[:, None]
    mask = (token_job_index[:, None] == lax.iota(jnp.int32, rank)[None, :] // ADAPTER_RANK).astype(F32)
    hs = [columns(hidden, group, 1) for group in groups]
    downs = [columns(down, [p for c in share for p in runs[c]], 0) for share in shares]
    downs = [jnp.concatenate([d] * 3, axis=1) for d in downs]
    lora_in = (jnp.dot(hidden, down, preferred_element_type=F32) * mask).astype(BF)
    hs, downs, mask, onehot, lora_in, local_label = lax.optimization_barrier(
        (hs, downs, mask, onehot, lora_in, local_label)
    )

    acc = None
    for k, group in enumerate(groups[:-1]):
        acc = forward_group(acc, hs[k], [have[p] for p in group], (lora_in, up) if k == 0 else None)
    logits, e, own = finish_forward(acc, hs[-1], [have[p] for p in groups[-1]], local_label, weight)

    def join(a, b):
        top = jnp.maximum(a[0:1], b[0:1])
        s = a[1:2] * jnp.exp(a[0:1] - top) + b[1:2] * jnp.exp(b[0:1] - top)
        return jnp.concatenate([top, s, a[2:3] + b[2:3], jnp.zeros((5, wide), F32)], axis=0)

    joint, bit = own, 1
    while bit < m:
        other = swap(joint, "vocab", m, bit)
        joint = join(joint, other)
        bit *= 2
    row_max, exp_total, target = joint[0, :t], joint[1, :t], joint[2, :t]
    token_loss = row_max + jnp.log(exp_total) - target

    terms = []
    for k, share in enumerate(shares):
        pieces = [have[p] for c in share for p in runs[c]]
        sizes = [sum(p[2] for p in runs[c]) for c in share]
        if k == 0:
            grad, again, lg, *terms = gradient_and_chunks(
                e, local_label, own, joint, up, mask, pieces, downs[0], sizes
            )
        else:
            terms += column_chunks(again, lg, pieces, downs[k], sizes)

    inward = m // 2 - 1
    out = jnp.zeros((t, width), BF)
    for part, run in zip(terms, runs):
        for s in range(inward):
            got = lax.ppermute(part, "vocab", [(s, s + 1), (m - 1 - s, m - 2 - s)])
            part = part + got
        got = lax.ppermute(part, "vocab", [(m // 2 - 1, m // 2), (m // 2, m // 2 - 1)])
        part = part + got
        for s in reversed(range(inward)):
            got = lax.ppermute(part, "vocab", [(s + 1, s), (m - 2 - s, m - 1 - s)])
            part = jnp.where((z == s) | (z == m - 1 - s), got, part)
        at = 0
        for r, s, length in run:
            out = lax.dynamic_update_slice_in_dim(
                out, part[:, at:at + length], (me ^ r) * rows + s, axis=1
            )
            at += length

    job_sums = jnp.sum(onehot * token_loss[:, None], axis=0)
    for bit in bits[:1] + bits[:0:-1]:
        other = swap(job_sums, "dp", n, bit)
        job_sums = job_sums + other
    job_sums, counts = lax.optimization_barrier((job_sums, counts))
    job_loss = job_sums / jnp.maximum(counts, 1.0)
    return logits, grad, out, token_loss, job_loss


def solution(mesh):
    in_specs = (P("dp", None), P("dp", "vocab"), P(), P(None, "vocab"), P("dp"), P("dp"))
    out_specs = (P("dp", "vocab"), P("dp", "vocab"), P("dp", None), P("dp"), P())
    return jax.shard_map(program, mesh=mesh, in_specs=in_specs, out_specs=out_specs, check_vma=False)
```
